256 devices in a mesh: nest: 4 (over y), tile: 64 (over z, x, core).
Axes of the slice: x: 4, y: 4, z: 8, core: 2. Of those that a mesh axis runs over, the one named last changes fastest.
Arguments:
- child_fields: float32 [4, 32, 1536, 3072], P('nest', None, 'tile'), may hold values from -18 to 18
- row_weights: float32 [8, 24], replicated
- col_weights: float32 [3072, 1024], replicated
- nest_offsets: int32 [4, 2], replicated, may hold values from 0 to 1023, as said below
- priority: int32 [1024, 1024], P('tile', 'nest'), may hold values from -1 to 3, as said below
- parent_old: float32 [32, 1024, 1024], P(None, 'tile', 'nest'), may hold values from -6 to 6
- smooth_rate: float32 [32], replicated, may hold values from 0.03 to 0.22
Outputs:
- parent_new: float32 [32, 1024, 1024], P(None, 'tile', 'nest')
The draws below stay inside these ranges and needn't reach their ends.
Inputs may be any that keep to these rules, and one draw needn't show every extreme that they name: nest_offsets[n, 0] lies in 0 .. 512 and nest_offsets[n, 1] in 0 .. 1023. priority[x, y] is -1 or a nest n with nest_offsets[n, 0] <= y < nest_offsets[n, 0] + 512.
All inputs are finite; a program needn't handle non-finite values.
Results may differ from the reference program's by a relative error of at most 0.000058.
Values sent between devices are 32-bit elements; how exact they have to be, the bound alone decides.
A program may use at most 128 MiB of HBM per device.

```python
import math
import jax
import jax.numpy as jnp
from jax import lax

CROW = 24
FL = 32
PRD = 8
PCOLS = 1024
CW = 3072
CROWS_ALL = 1536
NR = 512
PROWS_ALL = 1024
NESTS = 4


def nest_layout(key):
    key_top, key_left, key_score, key_skip, key_order = jax.random.split(jax.random.fold_in(key, 7), 5)
    top_rows = jax.random.randint(key_top, (NESTS,), 0, PROWS_ALL - NR + 1)
    left_cols = jax.random.randint(key_left, (NESTS,), 0, PCOLS)
    order = jax.random.permutation(key_order, NESTS)
    top_rows = top_rows.at[order[0]].set(PROWS_ALL - NR)
    top_rows = top_rows.at[order[1 % NESTS]].set(0)
    left_cols = left_cols.at[order[2 % NESTS]].set(PCOLS - 1)
    left_cols = left_cols.at[order[3 % NESTS]].set(0)
    row_ids = jnp.arange(PROWS_ALL)
    covered = (row_ids[None, :] >= top_rows[:, None]) & (row_ids[None, :] < top_rows[:, None] + NR)
    scores = jax.random.randint(key_score, (NESTS, PCOLS, PROWS_ALL), 0, 1000) * NESTS + jnp.arange(NESTS)[:, None, None]
    scores = jnp.where(covered[:, None, :], scores, -1)
    chosen = jnp.argmax(scores, axis=0).astype(jnp.int32)
    any_cover = jnp.any(covered, axis=0)
    skipped = jax.random.randint(key_skip, (PCOLS, PROWS_ALL), 0, 4) == 0
    priority_map = jnp.where(any_cover[None, :] & jnp.logical_not(skipped), chosen, -1)
    offsets = jnp.stack([top_rows, left_cols], axis=1)
    return (offsets.astype(jnp.int32), priority_map.astype(jnp.int32))


def draw_nest_offsets(key, part):
    return nest_layout(key)[0]


def draw_priority(key, part):
    return nest_layout(key)[1]


def draw_row_weights(key, part):
    tap_weights = jax.random.uniform(key, (PRD, 3), jnp.float32, 0.5, 1.5)
    tap_weights = tap_weights / jnp.sum(tap_weights, axis=1, keepdims=True)
    col_ids = jnp.arange(CROW)
    parent_ids = jnp.arange(PRD)
    matrix = jnp.zeros((PRD, CROW), jnp.float32)
    for member in range(3):
        matrix = matrix + tap_weights[:, member:member + 1] * (col_ids[None, :] == 3 * parent_ids[:, None] + member).astype(jnp.float32)
    return matrix


def draw_col_weights(key, part):
    key_inner, key_outer = jax.random.split(key)
    inner = jax.random.uniform(key_inner, (PCOLS, 3), jnp.float32, 0.5, 1.5)
    outer = jax.random.uniform(key_outer, (PCOLS, 2), jnp.float32, 0.1, 0.5)
    tap_weights = jnp.concatenate([outer[:, :1], inner, outer[:, 1:]], axis=1)
    tap_weights = tap_weights / jnp.sum(tap_weights, axis=1, keepdims=True)
    child_ids = jnp.arange(CW)
    parent_ids = jnp.arange(PCOLS)
    matrix = jnp.zeros((CW, PCOLS), jnp.float32)
    for member in range(5):
        target = (3 * parent_ids + member - 1) % CW
        matrix = matrix + tap_weights[None, :, member] * (child_ids[:, None] == target[None, :]).astype(jnp.float32)
    return matrix


def block_levels(key, extent, pieces, smallest, largest):
    loudness, own = 1.0, jax.random.fold_in(key, 6)
    for dim, shards_of in pieces:
        heights = jnp.exp(jax.random.uniform(jax.random.fold_in(own, dim), (shards_of,), jnp.float32, smallest / len(pieces), largest / len(pieces)))
        loudness = loudness * jnp.repeat(heights, extent[dim] // shards_of).reshape([-1 if axis == dim else 1 for axis in range(len(extent))])
    return loudness


def normal_values(key, dims, deviation, limit, cuts=(), kind=jnp.bfloat16):
    gain = block_levels(key, dims, cuts, -0.22, 0.18) if cuts else 1.0
    entries = jax.random.normal(key, dims, jnp.float32) * deviation * gain
    return jnp.minimum(jnp.maximum(entries, -limit), limit).astype(kind)


def setup_inputs(seed: int = 0) -> dict:
    key_list = jax.random.split(jax.random.key(seed), 8)
    child_fields = normal_values(key_list[0], (NESTS, FL, CROWS_ALL, CW), 3.0, 18.0, ((0, 4), (2, 64)), jnp.float32)
    row_weights = draw_row_weights(jax.random.fold_in(key_list[7], 71), 0)
    col_weights = draw_col_weights(jax.random.fold_in(key_list[7], 71), 0)
    nest_offsets = draw_nest_offsets(jax.random.fold_in(key_list[7], 71), 0)
    priority = draw_priority(jax.random.fold_in(key_list[7], 71), 0)
    parent_old = normal_values(key_list[5], (FL, PCOLS, PROWS_ALL), 1.0, 6.0, ((1, 64), (2, 4)), jnp.float32)
    smooth_rate = jnp.clip(jnp.exp(jax.random.uniform(key_list[6], (FL,), jnp.float32, math.log(0.03), math.log(0.22))), 0.03, 0.22)
    return {"child_fields": child_fields, "row_weights": row_weights, "col_weights": col_weights, "nest_offsets": nest_offsets, "priority": priority, "parent_old": parent_old, "smooth_rate": smooth_rate}


def reference(child_fields, row_weights, col_weights, nest_offsets, priority, parent_old, smooth_rate):
    nest_count, planes, crows_all, child_cols = child_fields.shape
    cell_rows, child_rows = row_weights.shape
    row_blocks = crows_all // child_rows
    nrows = row_blocks * cell_rows

    def restrict_one(child_block):
        grouped = child_block.reshape(planes, row_blocks, child_rows, child_cols)
        thinned = jnp.einsum('pr,ftrc->ftpc', row_weights, grouped, precision=lax.Precision.HIGHEST)
        thinned = thinned.reshape(planes, nrows, child_cols)
        return jnp.einsum('fyc,cx->fxy', thinned, col_weights, precision=lax.Precision.HIGHEST)

    restricted = lax.map(restrict_one, child_fields)
    merged = parent_old
    for nest_num in range(nest_count):
        rolled = jnp.roll(restricted[nest_num], nest_offsets[nest_num, 1], axis=1)
        placed = lax.dynamic_update_slice(jnp.zeros_like(parent_old), rolled,
                                          (jnp.int32(0), jnp.int32(0), nest_offsets[nest_num, 0].astype(jnp.int32)))
        merged = jnp.where((priority == nest_num)[None], placed, merged)
    east_side = jnp.roll(merged, -1, axis=1)
    west_side = jnp.roll(merged, 1, axis=1)
    padded = jnp.concatenate([merged[:, :, :1], merged, merged[:, :, -1:]], axis=2)
    north_side = padded[:, :, 2:]
    south_side = padded[:, :, :-2]
    return merged + smooth_rate[:, None, None] * (east_side + west_side + north_side + south_side - 4.0 * merged)
```

```python
import functools

import jax
import jax.numpy as jnp
from jax import lax
from jax.experimental import pallas as pl
from jax.experimental.pallas import tpu as pltpu
from jax.sharding import PartitionSpec as P

MESH = pl.DeviceIdType.MESH
TILES = 64
NESTS = 4
GROUPS = 4
GF = 8
PR = 8
STRIP = 16
LANES = 128
NROWS = 512
OWN = 256
DEPTH = 512


def split(value):
    high = value.astype(jnp.bfloat16)
    low = (value - high.astype(jnp.float32)).astype(jnp.bfloat16)
    return high, low


def dot(a, b):
    return jnp.dot(a, b, preferred_element_type=jnp.float32)


def block_diagonal(weights, fields):
    rows, depth = weights.shape
    shape = (fields * rows, fields * depth)
    left = lax.broadcasted_iota(jnp.int32, (shape[0], rows), 0) % rows
    left = (left == lax.broadcasted_iota(jnp.int32, (shape[0], rows), 1)).astype(jnp.bfloat16)
    right = lax.broadcasted_iota(jnp.int32, (depth, shape[1]), 1) % depth
    right = (right == lax.broadcasted_iota(jnp.int32, (depth, shape[1]), 0)).astype(jnp.bfloat16)
    same = lax.broadcasted_iota(jnp.int32, shape, 0) // rows == lax.broadcasted_iota(jnp.int32, shape, 1) // depth
    spread = dot(dot(left, weights).astype(jnp.bfloat16), right)
    return jnp.where(same, spread, 0.0).astype(jnp.bfloat16)


def regroup(tiles):
    group = lax.broadcasted_iota(jnp.int32, (PR, LANES), 1) // STRIP
    for step in (1, 2, 4):
        keep = (group & step) == 0
        for i in range(GF):
            if i & step == 0:
                a, b = tiles[i], tiles[i + step]
                tiles[i] = jnp.where(keep, a, pltpu.roll(b, STRIP * step, 1))
                tiles[i + step] = jnp.where(keep, pltpu.roll(a, LANES - STRIP * step, 1), b)
    return tiles


def restrict_kernel(shift_ref, child_ref, rw_ref, cw_ref, out_ref, total, rolled):
    step = pl.program_id(0)
    w_high, w_low = split(rw_ref[...])
    w_high, w_low = block_diagonal(w_high, GF), block_diagonal(w_low, GF)
    thin = []
    for g in range(GROUPS):
        c_high, c_low = split(child_ref[pl.ds(g * GF, GF)].reshape(GF * 24, DEPTH))
        thin.append(dot(w_high, c_high) + (dot(w_low, c_high) + dot(w_high, c_low)))
    t_high, t_low = split(jnp.concatenate(thin, axis=0))
    m_high, m_low = split(cw_ref[...])
    part = dot(t_high, m_high) + (dot(t_low, m_high) + dot(t_high, m_low))

    @pl.when(step == 0)
    def _():
        total[...] = part

    @pl.when(step > 0)
    def _():
        total[...] += part

    @pl.when(step == pl.num_programs(0) - 1)
    def _():
        rolled[...] = pltpu.roll(total[...], shift_ref[0], 1)

        @pl.loop(0, GROUPS)
        def _(g):
            for z in range(8):
                tiles = [
                    rolled[pl.ds(pl.multiple_of((g * GF + f) * PR, PR), PR), z * LANES : (z + 1) * LANES]
                    for f in range(GF)
                ]
                for s, tile in enumerate(regroup(tiles)):
                    out_ref[z * 8 + s, g] = tile


def exchange_kernel(
    rate_ref, offsets_ref, sent, priority_ref, old_ref, out_ref,
    slabs, halves, nests, merged, mask, edges, rows_in, edges_in,
    tile_send, tile_recv, nest_send, nest_recv, halo_send, halo_recv,
):
    me, nest = lax.axis_index("tile"), lax.axis_index("nest")
    barrier = pltpu.get_barrier_semaphore()

    @pl.loop(1, TILES)
    def _(d):
        pl.semaphore_signal(barrier, inc=1, device_id={"tile": lax.rem(me + d, TILES)}, device_id_type=MESH)

    for d in range(1, NESTS):
        pl.semaphore_signal(barrier, inc=1, device_id={"nest": lax.rem(nest + d, NESTS)}, device_id_type=MESH)
    pl.semaphore_wait(barrier, TILES - 1 + NESTS - 1)

    own_rows = pl.ds(pl.multiple_of(me * PR, PR), PR)
    for g in range(GROUPS):
        @pl.loop(1, TILES)
        def _(d):
            peer = lax.rem(me + d, TILES)
            pltpu.make_async_remote_copy(
                src_ref=sent.at[peer, g], dst_ref=slabs[g].at[own_rows],
                send_sem=tile_send.at[g], recv_sem=tile_recv.at[g],
                device_id={"tile": peer}, device_id_type=MESH,
            ).start()

    for g in range(GROUPS):
        slabs[g][own_rows, :] = sent[me, g]

    spread = jnp.concatenate([priority_ref[...].astype(jnp.float32)] * GF, axis=0)
    mask[...] = spread.T
    for g in range(GROUPS):
        merged[g] = old_ref[pl.ds(g * GF, GF)].reshape(LANES, OWN).T

    def wait(ref, sem):
        pltpu.make_async_copy(ref, ref, sem).wait()

    first = offsets_ref[nest, 0]
    half = lax.rem(nest, 2)

    def nest_copy(g, d):
        peer = lax.rem(nest + d, NESTS)
        return pltpu.make_async_remote_copy(
            src_ref=halves.at[g, pl.ds(pl.multiple_of(lax.rem(peer, 2) * OWN, OWN), OWN)],
            dst_ref=nests.at[nest, g],
            send_sem=nest_send.at[g, d], recv_sem=nest_recv.at[g, d],
            device_id={"nest": peer}, device_id_type=MESH,
        )

    for g in range(GROUPS):
        wait(slabs[g].at[pl.ds(0, NROWS - PR)], tile_recv.at[g])
        slab = slabs[g]
        slab[NROWS : NROWS + PR, :] = slab[0:PR, :]

        @pl.loop(0, NROWS // PR)
        def _(b):
            start = (b * PR - first) & (NROWS - 1)
            halves[g, pl.ds(pl.multiple_of(b * PR, PR), PR), :] = slab[pl.ds(start, PR), :]

        for d in range(1, NESTS):
            nest_copy(g, d).start()
        nests[nest, g] = halves[g, pl.ds(pl.multiple_of(half * OWN, OWN), OWN), :]

    lane = lax.broadcasted_iota(jnp.int32, (STRIP, LANES), 1)
    column = lane % STRIP
    east, west = lax.rem(me + 1, TILES), lax.rem(me + TILES - 1, TILES)
    above, below = lax.rem(nest + 1, NESTS), lax.rem(nest + NESTS - 1, NESTS)

    def halo_copies(g):
        def copy(src, dst, k, device):
            return pltpu.make_async_remote_copy(
                src_ref=src, dst_ref=dst, send_sem=halo_send.at[g, k], recv_sem=halo_recv.at[g, k],
                device_id=device, device_id_type=MESH,
            )
        return [
            copy(edges.at[0, g], edges_in.at[0, g], 0, {"tile": east}),
            copy(edges.at[1, g], edges_in.at[1, g], 1, {"tile": west}),
            copy(merged.at[g, pl.ds(OWN - PR, PR)], rows_in.at[0, g], 2, {"nest": above}),
            copy(merged.at[g, pl.ds(0, PR)], rows_in.at[1, g], 3, {"nest": below}),
        ]

    for g in range(GROUPS):
        for d in range(1, NESTS):
            nest_copy(g, d).wait_recv()
        high = jnp.zeros((STRIP, LANES), jnp.float32)
        low = jnp.zeros((STRIP, LANES), jnp.float32)
        for b in range(OWN // STRIP):
            rows = slice(b * STRIP, (b + 1) * STRIP)
            chosen = merged[g, rows, :]
            which = mask[rows, :]
            for n in range(NESTS):
                chosen = jnp.where(which == n, nests[n, g, rows, :], chosen)
            merged[g, rows, :] = chosen
            to_high = pltpu.roll(chosen, (b - (STRIP - 1)) % LANES, 1)
            to_low = pltpu.roll(chosen, b, 1)
            high = jnp.where(column == b, to_high, high)
            low = jnp.where(column == b, to_low, low)
        edges[0, g] = high
        edges[1, g] = low
        for copy in halo_copies(g):
            copy.start()

    wide = lax.broadcasted_iota(jnp.int32, (OWN, LANES), 1)
    wide_column = wide % STRIP
    row = lax.broadcasted_iota(jnp.int32, (OWN, LANES), 0)
    for g in range(GROUPS):
        copies = halo_copies(g)
        for copy in copies:
            copy.wait_recv()
        cell = merged[g]
        from_west = edges_in[0, g]
        from_east = edges_in[1, g]
        west_edge = jnp.concatenate(
            [pltpu.roll(from_west, (-b) % LANES, 1) for b in range(OWN // STRIP)], axis=0
        )
        east_edge = jnp.concatenate(
            [pltpu.roll(from_east, (STRIP - 1 - b) % LANES, 1) for b in range(OWN // STRIP)], axis=0
        )
        west_side = jnp.where(wide_column == 0, west_edge, pltpu.roll(cell, 1, 1))
        east_side = jnp.where(wide_column == STRIP - 1, east_edge, pltpu.roll(cell, LANES - 1, 1))
        south_row = jnp.where(nest == 0, cell[0:1], rows_in[0, g, PR - 1 : PR])
        north_row = jnp.where(nest == NESTS - 1, cell[OWN - 1 : OWN], rows_in[1, g, 0:1])
        south_side = jnp.where(row == 0, south_row, pltpu.roll(cell, 1, 0))
        north_side = jnp.where(row == OWN - 1, north_row, pltpu.roll(cell, OWN - 1, 0))
        rate = jnp.full((1, LANES), rate_ref[g * GF], jnp.float32)
        for f in range(1, GF):
            rate = jnp.where(wide[0:1] // STRIP == f, rate_ref[g * GF + f], rate)
        new = cell + rate * (east_side + west_side + north_side + south_side - 4.0 * cell)
        out_ref[pl.ds(g * GF, GF)] = new.T.reshape(GF, STRIP, OWN)

    for g in range(GROUPS):
        wait(slabs[g].at[pl.ds(0, NROWS - PR)], tile_send.at[g])
        for d in range(1, NESTS):
            nest_copy(g, d).wait_send()
        for copy in halo_copies(g):
            copy.wait_send()


def per_device(child_fields, row_weights, col_weights, nest_offsets, priority, parent_old, smooth_rate):
    nest = lax.axis_index("nest")
    depth = col_weights.shape[0]
    vmem = pl.BlockSpec(memory_space=pltpu.VMEM)
    smem = pl.BlockSpec(memory_space=pltpu.SMEM)
    f32 = jnp.float32
    shift = lax.dynamic_slice(nest_offsets, (nest, 1), (1, 1)).reshape(1)
    sent = pl.pallas_call(
        restrict_kernel,
        grid=(depth // DEPTH,),
        out_shape=jax.ShapeDtypeStruct((TILES, GROUPS, PR, LANES), f32),
        in_specs=[
            smem,
            pl.BlockSpec((32, 24, DEPTH), lambda k: (0, 0, k)),
            pl.BlockSpec((8, 24), lambda k: (0, 0)),
            pl.BlockSpec((DEPTH, 1024), lambda k: (k, 0)),
        ],
        out_specs=pl.BlockSpec((TILES, GROUPS, PR, LANES), lambda k: (0, 0, 0, 0)),
        scratch_shapes=[pltpu.VMEM((256, 1024), f32), pltpu.VMEM((256, 1024), f32)],
        name="restrict",
        compiler_params=pltpu.CompilerParams(dimension_semantics=("arbitrary",)),
    )(shift, child_fields[0], row_weights, col_weights)
    dma = pltpu.SemaphoreType.DMA
    return pl.pallas_call(
        exchange_kernel,
        out_shape=jax.ShapeDtypeStruct(parent_old.shape, f32),
        in_specs=[smem, smem, vmem, vmem, vmem],
        out_specs=vmem,
        scratch_shapes=[
            [pltpu.VMEM((NROWS + PR, LANES), f32)] * GROUPS,
            pltpu.VMEM((GROUPS, NROWS, LANES), f32),
            pltpu.VMEM((NESTS, GROUPS, OWN, LANES), f32),
            pltpu.VMEM((GROUPS, OWN, LANES), f32),
            pltpu.VMEM((OWN, LANES), f32),
            pltpu.VMEM((2, GROUPS, STRIP, LANES), f32),
            pltpu.VMEM((2, GROUPS, PR, LANES), f32),
            pltpu.VMEM((2, GROUPS, STRIP, LANES), f32),
            dma((GROUPS,)), dma((GROUPS,)), dma((GROUPS, NESTS)), dma((GROUPS, NESTS)),
            dma((GROUPS, 4)), dma((GROUPS, 4)),
        ],
        name="exchange",
        compiler_params=pltpu.CompilerParams(collective_id=0, has_side_effects=True),
    )(smooth_rate, nest_offsets, sent, priority, parent_old)


def solution(mesh):
    return jax.shard_map(
        per_device,
        mesh=mesh,
        in_specs=(
            P("nest", None, "tile", None), P(), P(), P(), P("tile", "nest"), P(None, "tile", "nest"), P(),
        ),
        out_specs=P(None, "tile", "nest"),
        check_vma=False,
    )
```

```python
import functools

import jax
import jax.numpy as jnp
from jax import lax
from jax.experimental import pallas as pl
from jax.experimental.pallas import tpu as pltpu
from jax.sharding import PartitionSpec as P

MESH = pl.DeviceIdType.MESH
TILES = 64
NESTS = 4
GROUPS = 4
GF = 8
PR = 8
STRIP = 16
LANES = 128
NROWS = 512
OWN = 256
DEPTH = 512


def split(value):
    high = value.astype(jnp.bfloat16)
    low = (value - high.astype(jnp.float32)).astype(jnp.bfloat16)
    return high, low


def dot(a, b):
    return jnp.dot(a, b, preferred_element_type=jnp.float32)


def block_diagonal(weights, fields):
    rows, depth = weights.shape
    shape = (fields * rows, fields * depth)
    left = lax.broadcasted_iota(jnp.int32, (shape[0], rows), 0) % rows
    left = (left == lax.broadcasted_iota(jnp.int32, (shape[0], rows), 1)).astype(jnp.bfloat16)
    right = lax.broadcasted_iota(jnp.int32, (depth, shape[1]), 1) % depth
    right = (right == lax.broadcasted_iota(jnp.int32, (depth, shape[1]), 0)).astype(jnp.bfloat16)
    same = lax.broadcasted_iota(jnp.int32, shape, 0) // rows == lax.broadcasted_iota(jnp.int32, shape, 1) // depth
    spread = dot(dot(left, weights).astype(jnp.bfloat16), right)
    return jnp.where(same, spread, 0.0).astype(jnp.bfloat16)


def regroup(tiles):
    group = lax.broadcasted_iota(jnp.int32, (PR, LANES), 1) // STRIP
    for step in (1, 2, 4):
        keep = (group & step) == 0
        for i in range(GF):
            if i & step == 0:
                a, b = tiles[i], tiles[i + step]
                tiles[i] = jnp.where(keep, a, pltpu.roll(b, STRIP * step, 1))
                tiles[i + step] = jnp.where(keep, pltpu.roll(a, LANES - STRIP * step, 1), b)
    return tiles


def restrict_half(h, shift, waits, child, weights, high, low, total, packed):
    w_high, w_low = weights
    for c in range(3):
        waits[0][c].wait()
        columns = slice(c * 1024, (c + 1) * 1024)
        for g in range(2):
            c_high, c_low = split(child[0][pl.ds(h * 16 + g * GF, GF), :, columns].reshape(GF * 24, 1024))
            thin = dot(w_high, c_high) + (dot(w_low, c_high) + dot(w_high, c_low))
            t_high, t_low = split(thin)
            high[g * 64 : (g + 1) * 64, columns] = t_high
            low[g * 64 : (g + 1) * 64, columns] = t_low
    for k in range(3072 // DEPTH):
        rows = slice(k * DEPTH, (k + 1) * DEPTH)
        if waits[1]:
            waits[1][k].wait()
        m_high, m_low = split(child[1][rows, :])
        part = dot(high[:, rows], m_high) + (dot(low[:, rows], m_high) + dot(high[:, rows], m_low))
        if k == 0:
            total[...] = part
        else:
            total[...] += part
    total[...] = pltpu.roll(total[...], shift, 1)
    for g in range(2):
        for z in range(8):
            tiles = [total[(g * GF + f) * PR : (g * GF + f + 1) * PR, z * LANES : (z + 1) * LANES] for f in range(GF)]
            for s, tile in enumerate(regroup(tiles)):
                packed[z * 8 + s, h * 2 + g] = tile


def step_kernel(
    rate_ref, offsets_ref, child_hbm, rw_ref, cw_hbm, priority_ref, old_ref, out_ref,
    child, cw, high, low, total, sent,
    slabs, halves, nests, merged, mask, edges, rows_in, edges_in,
    child_sem, cw_sem, tile_send, tile_recv, nest_send, nest_recv, halo_send, halo_recv,
):
    me, nest = lax.axis_index("tile"), lax.axis_index("nest")
    barrier = pltpu.get_barrier_semaphore()

    def child_copy(h, c):
        part = (pl.ds(h * 16, 16), slice(None), pl.ds(c * 1024, 1024))
        return pltpu.make_async_copy(child_hbm.at[part], child.at[part], child_sem.at[h, c])

    def cw_copy(k):
        rows = pl.ds(k * DEPTH, DEPTH)
        return pltpu.make_async_copy(cw_hbm.at[rows], cw.at[rows], cw_sem.at[k])

    child_copies = [[child_copy(h, c) for c in range(3)] for h in range(2)]
    cw_copies = [cw_copy(k) for k in range(3072 // DEPTH)]
    for copy in child_copies[0] + cw_copies + child_copies[1]:
        copy.start()

    @pl.loop(1, TILES)
    def _(d):
        pl.semaphore_signal(barrier, inc=1, device_id={"tile": lax.rem(me + d, TILES)}, device_id_type=MESH)

    for d in range(1, NESTS):
        pl.semaphore_signal(barrier, inc=1, device_id={"nest": lax.rem(nest + d, NESTS)}, device_id_type=MESH)

    own_rows = pl.ds(pl.multiple_of(me * PR, PR), PR)

    def send_group(g):
        @pl.loop(1, TILES)
        def _(d):
            peer = lax.rem(me + d, TILES)
            pltpu.make_async_remote_copy(
                src_ref=sent.at[peer, g], dst_ref=slabs[g].at[own_rows],
                send_sem=tile_send.at[g], recv_sem=tile_recv.at[g],
                device_id={"tile": peer}, device_id_type=MESH,
            ).start()

    shift = offsets_ref[1, nest]
    r_high, r_low = split(rw_ref[...])
    weights = block_diagonal(r_high, GF), block_diagonal(r_low, GF)
    restrict_half(0, shift, (child_copies[0], cw_copies), (child, cw), weights, high, low, total, sent)
    pl.semaphore_wait(barrier, TILES - 1 + NESTS - 1)
    send_group(0)
    send_group(1)
    restrict_half(1, shift, (child_copies[1], None), (child, cw), weights, high, low, total, sent)
    send_group(2)
    send_group(3)

    for g in range(GROUPS):
        slabs[g][own_rows, :] = sent[me, g]

    spread = jnp.concatenate([priority_ref[...].astype(jnp.float32)] * GF, axis=0)
    mask[...] = spread.T
    for g in range(GROUPS):
        merged[g] = old_ref[pl.ds(g * GF, GF)].reshape(LANES, OWN).T

    def wait(ref, sem):
        pltpu.make_async_copy(ref, ref, sem).wait()

    first = offsets_ref[0, nest]
    half = lax.rem(nest, 2)

    def nest_copy(g, d):
        peer = lax.rem(nest + d, NESTS)
        return pltpu.make_async_remote_copy(
            src_ref=halves.at[g, pl.ds(pl.multiple_of(lax.rem(peer, 2) * OWN, OWN), OWN)],
            dst_ref=nests.at[nest, g],
            send_sem=nest_send.at[g, d], recv_sem=nest_recv.at[g, d],
            device_id={"nest": peer}, device_id_type=MESH,
        )

    def shift_rows(g):
        slab = slabs[g]
        wait(slab.at[pl.ds(0, NROWS - PR)], tile_recv.at[g])
        slab[NROWS : NROWS + PR, :] = slab[0:PR, :]
        for b in range(NROWS // PR):
            start = (b * PR - first) & (NROWS - 1)
            halves[g, b * PR : (b + 1) * PR, :] = slab[pl.ds(start, PR), :]
        for d in range(1, NESTS):
            nest_copy(g, d).start()
        nests[nest, g] = halves[g, pl.ds(pl.multiple_of(half * OWN, OWN), OWN), :]

    lane = lax.broadcasted_iota(jnp.int32, (STRIP, LANES), 1)
    column = lane % STRIP
    east, west = lax.rem(me + 1, TILES), lax.rem(me + TILES - 1, TILES)
    above, below = lax.rem(nest + 1, NESTS), lax.rem(nest + NESTS - 1, NESTS)

    def halo_copies(g):
        def copy(src, dst, k, device):
            return pltpu.make_async_remote_copy(
                src_ref=src, dst_ref=dst, send_sem=halo_send.at[g, k], recv_sem=halo_recv.at[g, k],
                device_id=device, device_id_type=MESH,
            )
        return [
            copy(edges.at[0, g], edges_in.at[0, g], 0, {"tile": east}),
            copy(edges.at[1, g], edges_in.at[1, g], 1, {"tile": west}),
            copy(merged.at[g, pl.ds(OWN - PR, PR)], rows_in.at[0, g], 2, {"nest": above}),
            copy(merged.at[g, pl.ds(0, PR)], rows_in.at[1, g], 3, {"nest": below}),
        ]

    def merge(g):
        for d in range(1, NESTS):
            nest_copy(g, d).wait_recv()
        high = jnp.zeros((STRIP, LANES), jnp.float32)
        low = jnp.zeros((STRIP, LANES), jnp.float32)
        for b in range(OWN // STRIP):
            rows = slice(b * STRIP, (b + 1) * STRIP)
            chosen = merged[g, rows, :]
            which = mask[rows, :]
            for n in range(NESTS):
                chosen = jnp.where(which == n, nests[n, g, rows, :], chosen)
            merged[g, rows, :] = chosen
            to_high = pltpu.roll(chosen, (b - (STRIP - 1)) % LANES, 1)
            to_low = pltpu.roll(chosen, b, 1)
            high = jnp.where(column == b, to_high, high)
            low = jnp.where(column == b, to_low, low)
        edges[0, g] = high
        edges[1, g] = low
        for copy in halo_copies(g):
            copy.start()

    wide = lax.broadcasted_iota(jnp.int32, (OWN, LANES), 1)
    wide_column = wide % STRIP
    row = lax.broadcasted_iota(jnp.int32, (OWN, LANES), 0)
    def smooth(g):
        copies = halo_copies(g)
        for copy in copies:
            copy.wait_recv()
        cell = merged[g]
        from_west = edges_in[0, g]
        from_east = edges_in[1, g]
        west_edge = jnp.concatenate(
            [pltpu.roll(from_west, (-b) % LANES, 1) for b in range(OWN // STRIP)], axis=0
        )
        east_edge = jnp.concatenate(
            [pltpu.roll(from_east, (STRIP - 1 - b) % LANES, 1) for b in range(OWN // STRIP)], axis=0
        )
        west_side = jnp.where(wide_column == 0, west_edge, pltpu.roll(cell, 1, 1))
        east_side = jnp.where(wide_column == STRIP - 1, east_edge, pltpu.roll(cell, LANES - 1, 1))
        south_row = jnp.where(nest == 0, cell[0:1], rows_in[0, g, PR - 1 : PR])
        north_row = jnp.where(nest == NESTS - 1, cell[OWN - 1 : OWN], rows_in[1, g, 0:1])
        south_side = jnp.where(row == 0, south_row, pltpu.roll(cell, 1, 0))
        north_side = jnp.where(row == OWN - 1, north_row, pltpu.roll(cell, OWN - 1, 0))
        rate = jnp.full((1, LANES), rate_ref[g * GF], jnp.float32)
        for f in range(1, GF):
            rate = jnp.where(wide[0:1] // STRIP == f, rate_ref[g * GF + f], rate)
        new = cell + rate * (east_side + west_side + north_side + south_side - 4.0 * cell)
        out_ref[pl.ds(g * GF, GF)] = new.T.reshape(GF, STRIP, OWN)

    for g in range(GROUPS):
        shift_rows(g)
        if g >= 1:
            merge(g - 1)
        if g >= 2:
            smooth(g - 2)
    merge(GROUPS - 1)
    smooth(GROUPS - 2)
    smooth(GROUPS - 1)

    for g in range(GROUPS):
        wait(slabs[g].at[pl.ds(0, NROWS - PR)], tile_send.at[g])
        for d in range(1, NESTS):
            nest_copy(g, d).wait_send()
        for copy in halo_copies(g):
            copy.wait_send()


def per_device(child_fields, row_weights, col_weights, nest_offsets, priority, parent_old, smooth_rate):
    vmem = pl.BlockSpec(memory_space=pltpu.VMEM)
    smem = pl.BlockSpec(memory_space=pltpu.SMEM)
    hbm = pl.BlockSpec(memory_space=pl.ANY)
    f32, bf16 = jnp.float32, jnp.bfloat16
    dma = pltpu.SemaphoreType.DMA
    return pl.pallas_call(
        step_kernel,
        out_shape=jax.ShapeDtypeStruct(parent_old.shape, f32),
        in_specs=[smem, smem, hbm, vmem, hbm, vmem, vmem],
        out_specs=vmem,
        scratch_shapes=[
            pltpu.VMEM((32, 24, 3072), f32),
            pltpu.VMEM((3072, 1024), f32),
            pltpu.VMEM((128, 3072), bf16),
            pltpu.VMEM((128, 3072), bf16),
            pltpu.VMEM((128, 1024), f32),
            pltpu.VMEM((TILES, GROUPS, PR, LANES), f32),
            [pltpu.VMEM((NROWS + PR, LANES), f32)] * GROUPS,
            pltpu.VMEM((GROUPS, NROWS, LANES), f32),
            pltpu.VMEM((NESTS, GROUPS, OWN, LANES), f32),
            pltpu.VMEM((GROUPS, OWN, LANES), f32),
            pltpu.VMEM((OWN, LANES), f32),
            pltpu.VMEM((2, GROUPS, STRIP, LANES), f32),
            pltpu.VMEM((2, GROUPS, PR, LANES), f32),
            pltpu.VMEM((2, GROUPS, STRIP, LANES), f32),
            dma((2, 3)), dma((3072 // DEPTH,)),
            dma((GROUPS,)), dma((GROUPS,)), dma((GROUPS, NESTS)), dma((GROUPS, NESTS)),
            dma((GROUPS, 4)), dma((GROUPS, 4)),
        ],
        name="feedback",
        compiler_params=pltpu.CompilerParams(collective_id=0, has_side_effects=True),
    )(smooth_rate, nest_offsets.T, child_fields[0], row_weights, col_weights, priority, parent_old)


def solution(mesh):
    return jax.shard_map(
        per_device,
        mesh=mesh,
        in_specs=(
            P("nest", None, "tile", None), P(), P(), P(), P("tile", "nest"), P(None, "tile", "nest"), P(),
        ),
        out_specs=P(None, "tile", "nest"),
        check_vma=False,
    )
```

```python
import functools

import jax
import jax.numpy as jnp
from jax import lax
from jax.experimental import pallas as pl
from jax.experimental.pallas import tpu as pltpu
from jax.sharding import PartitionSpec as P

MESH = pl.DeviceIdType.MESH
TILES = 64
NESTS = 4
GROUPS = 4
GF = 8
PR = 8
STRIP = 16
PASSES = ((0,), (1,), (2, 3))
LANES = 128
NROWS = 512
OWN = 256
DEPTH = 512
CHUNKS = tuple((k, 512) for k in range(0, 3072, 512))


def split(value):
    high = value.astype(jnp.bfloat16)
    low = (value - high.astype(jnp.float32)).astype(jnp.bfloat16)
    return high, low


def dot(a, b):
    return jnp.dot(a, b, preferred_element_type=jnp.float32)


def block_diagonal(weights, fields):
    rows, depth = weights.shape
    shape = (fields * rows, fields * depth)
    left = lax.broadcasted_iota(jnp.int32, (shape[0], rows), 0) % rows
    left = (left == lax.broadcasted_iota(jnp.int32, (shape[0], rows), 1)).astype(jnp.bfloat16)
    right = lax.broadcasted_iota(jnp.int32, (depth, shape[1]), 1) % depth
    right = (right == lax.broadcasted_iota(jnp.int32, (depth, shape[1]), 0)).astype(jnp.bfloat16)
    same = lax.broadcasted_iota(jnp.int32, shape, 0) // rows == lax.broadcasted_iota(jnp.int32, shape, 1) // depth
    spread = dot(dot(left, weights).astype(jnp.bfloat16), right)
    return jnp.where(same, spread, 0.0).astype(jnp.bfloat16)


def regroup(tiles):
    group = lax.broadcasted_iota(jnp.int32, (PR, LANES), 1) // STRIP
    for step in (1, 2, 4):
        keep = (group & step) == 0
        for i in range(GF):
            if i & step == 0:
                a, b = tiles[i], tiles[i + step]
                tiles[i] = jnp.where(keep, a, pltpu.roll(b, STRIP * step, 1))
                tiles[i + step] = jnp.where(keep, pltpu.roll(a, LANES - STRIP * step, 1), b)
    return tiles


def restrict(groups, shift, child_waits, cw_waits, child, cw, weights, both, total, packed):
    count = len(groups) * GF * PR
    for c in range(3):
        columns = slice(c * 1024, (c + 1) * 1024)
        for i, g in enumerate(groups):
            child_waits[g][c].wait()
            c_high, c_low = split(child[pl.ds(g * GF, GF), :, columns].reshape(GF * 24, 1024))
            wide = dot(weights, c_high)
            t_high, t_low = split(wide[:64] + (wide[64:] + dot(weights[:64], c_low)))
            both[i * 64 : (i + 1) * 64, columns] = t_high
            both[count + i * 64 : count + (i + 1) * 64, columns] = t_low
    for start, depth in CHUNKS:
        rows = slice(start, start + depth)
        for copy, low, _ in cw_waits:
            if start <= low < start + depth:
                copy.wait()
        m_high, m_low = split(cw[rows, :])
        wide = dot(both[0 : 2 * count, rows], m_high)
        part = wide[:count] + (wide[count:] + dot(both[0:count, rows], m_low))
        if start == 0:
            total[0:count, :] = part
        else:
            total[0:count, :] += part
    total[0:count, :] = pltpu.roll(total[0:count, :], shift, 1)
    for i, g in enumerate(groups):
        for z in range(8):
            tiles = [total[(i * GF + f) * PR : (i * GF + f + 1) * PR, z * LANES : (z + 1) * LANES] for f in range(GF)]
            for s, tile in enumerate(regroup(tiles)):
                packed[z * 8 + s, g] = tile


def step_kernel(
    rate_hbm, offsets_hbm, child_hbm, rw_hbm, cw_hbm, priority_hbm, old_hbm, out_hbm,
    child, cw, both, total, sent, priority_ref, old_ref, out_ref, rate_ref, offsets_ref, rw_ref,
    slabs, halves, nests, merged, mask, edges, rows_in, edges_in,
    child_sem, cw_sem, own_sem, out_sem, tile_send, tile_recv, nest_send, nest_recv, halo_send, halo_recv,
):
    me, nest = lax.axis_index("tile"), lax.axis_index("nest")
    barrier = pltpu.get_barrier_semaphore()

    def child_copy(g, c):
        part = (pl.ds(g * GF, GF), slice(None), pl.ds(c * 1024, 1024))
        return pltpu.make_async_copy(child_hbm.at[part], child.at[part], child_sem.at[g, c])

    def cw_copy(k):
        rows = pl.ds(k * DEPTH, DEPTH)
        return pltpu.make_async_copy(cw_hbm.at[rows], cw.at[rows], cw_sem.at[k])

    child_copies = [[child_copy(g, c) for c in range(3)] for g in range(GROUPS)]
    cw_copies = [cw_copy(k) for k in range(3072 // DEPTH)]
    own_copies = [
        pltpu.make_async_copy(priority_hbm, priority_ref, own_sem.at[0]),
        pltpu.make_async_copy(old_hbm, old_ref, own_sem.at[1]),
    ]
    rate_copy = pltpu.make_async_copy(rate_hbm, rate_ref, own_sem.at[2])
    offsets_copy = pltpu.make_async_copy(offsets_hbm, offsets_ref, own_sem.at[3])
    rw_copy = pltpu.make_async_copy(rw_hbm, rw_ref, own_sem.at[4])
    for copy in (rw_copy, offsets_copy, rate_copy):
        copy.start()
    for copy in child_copies[0] + cw_copies + sum(child_copies[1:], own_copies):
        copy.start()

    @pl.loop(1, TILES)
    def _(d):
        pl.semaphore_signal(barrier, inc=1, device_id={"tile": lax.rem(me + d, TILES)}, device_id_type=MESH)

    for d in range(1, NESTS):
        pl.semaphore_signal(barrier, inc=1, device_id={"nest": lax.rem(nest + d, NESTS)}, device_id_type=MESH)

    own_rows = pl.ds(pl.multiple_of(me * PR, PR), PR)

    plane, seat = lax.div(me, 8), lax.rem(me, 8)

    def send_tile(g, peer):
        pltpu.make_async_remote_copy(
            src_ref=sent.at[peer, g], dst_ref=slabs[g].at[own_rows],
            send_sem=tile_send.at[g], recv_sem=tile_recv.at[g],
            device_id={"tile": peer}, device_id_type=MESH,
        ).start()

    def send_group(g):
        @pl.loop(0, 8)
        def _(d):
            for dz in (4, 3, 5, 2, 6, 1, 7):
                send_tile(g, lax.rem(plane + dz, 8) * 8 + lax.rem(seat + d, 8))

        @pl.loop(1, 8)
        def _(d):
            send_tile(g, plane * 8 + lax.rem(seat + d, 8))

    for copy in (rw_copy, offsets_copy, rate_copy):
        copy.wait()
    shift = offsets_ref[1, nest]
    r_high, r_low = split(rw_ref[...])
    weights = jnp.concatenate([block_diagonal(r_high, GF), block_diagonal(r_low, GF)], axis=0)
    cw_waits = [(copy, k * DEPTH, (k + 1) * DEPTH) for k, copy in enumerate(cw_copies)]
    for groups in PASSES:
        restrict(groups, shift, child_copies, cw_waits, child, cw, weights, both, total, sent)
        if groups[0] == 0:
            pl.semaphore_wait(barrier, TILES - 1 + NESTS - 1)
        cw_waits = []
        for g in groups:
            send_group(g)

    for g in range(GROUPS):
        slabs[g][own_rows, :] = sent[me, g]

    for copy in own_copies:
        copy.wait()
    spread = jnp.concatenate([priority_ref[...].astype(jnp.float32)] * GF, axis=0)
    mask[...] = spread.T
    for g in range(GROUPS):
        merged[g] = old_ref[pl.ds(g * GF, GF)].reshape(LANES, OWN).T

    def wait(ref, sem):
        pltpu.make_async_copy(ref, ref, sem).wait()

    first = offsets_ref[0, nest]
    half = lax.rem(nest, 2)

    def nest_copy(g, d):
        peer = lax.rem(nest + d, NESTS)
        return pltpu.make_async_remote_copy(
            src_ref=halves.at[g, pl.ds(pl.multiple_of(lax.rem(peer, 2) * OWN, OWN), OWN)],
            dst_ref=nests.at[nest, g],
            send_sem=nest_send.at[g, d], recv_sem=nest_recv.at[g, d],
            device_id={"nest": peer}, device_id_type=MESH,
        )

    def out_copy(g):
        part = pl.ds(g * GF, GF)
        return pltpu.make_async_copy(out_ref.at[part], out_hbm.at[part], out_sem.at[g])

    def shift_rows(g):
        slab = slabs[g]
        wait(slab.at[pl.ds(0, NROWS - PR)], tile_recv.at[g])
        slab[NROWS : NROWS + PR, :] = slab[0:PR, :]
        for b in range(NROWS // PR):
            start = (b * PR - first) & (NROWS - 1)
            halves[g, b * PR : (b + 1) * PR, :] = slab[pl.ds(start, PR), :]
        for d in range(1, NESTS):
            nest_copy(g, d).start()
        nests[nest, g] = halves[g, pl.ds(pl.multiple_of(half * OWN, OWN), OWN), :]

    lane = lax.broadcasted_iota(jnp.int32, (STRIP, LANES), 1)
    column = lane % STRIP
    east, west = lax.rem(me + 1, TILES), lax.rem(me + TILES - 1, TILES)
    above, below = lax.rem(nest + 1, NESTS), lax.rem(nest + NESTS - 1, NESTS)

    def halo_copies(g):
        def copy(src, dst, k, device):
            return pltpu.make_async_remote_copy(
                src_ref=src, dst_ref=dst, send_sem=halo_send.at[g, k], recv_sem=halo_recv.at[g, k],
                device_id=device, device_id_type=MESH,
            )
        return [
            copy(edges.at[0, g], edges_in.at[0, g], 0, {"tile": east}),
            copy(edges.at[1, g], edges_in.at[1, g], 1, {"tile": west}),
            copy(merged.at[g, pl.ds(OWN - PR, PR)], rows_in.at[0, g], 2, {"nest": above}),
            copy(merged.at[g, pl.ds(0, PR)], rows_in.at[1, g], 3, {"nest": below}),
        ]

    def merge(g):
        for d in range(1, NESTS):
            nest_copy(g, d).wait_recv()
        high = jnp.zeros((STRIP, LANES), jnp.float32)
        low = jnp.zeros((STRIP, LANES), jnp.float32)
        for b in range(OWN // STRIP):
            rows = slice(b * STRIP, (b + 1) * STRIP)
            chosen = merged[g, rows, :]
            which = mask[rows, :]
            for n in range(NESTS):
                chosen = jnp.where(which == n, nests[n, g, rows, :], chosen)
            merged[g, rows, :] = chosen
            to_high = pltpu.roll(chosen, (b - (STRIP - 1)) % LANES, 1)
            to_low = pltpu.roll(chosen, b, 1)
            high = jnp.where(column == b, to_high, high)
            low = jnp.where(column == b, to_low, low)
        edges[0, g] = high
        edges[1, g] = low
        for copy in halo_copies(g):
            copy.start()

    wide = lax.broadcasted_iota(jnp.int32, (OWN, LANES), 1)
    wide_column = wide % STRIP
    row = lax.broadcasted_iota(jnp.int32, (OWN, LANES), 0)
    def smooth(g):
        copies = halo_copies(g)
        for copy in copies:
            copy.wait_recv()
        cell = merged[g]
        from_west = edges_in[0, g]
        from_east = edges_in[1, g]
        west_edge = jnp.concatenate(
            [pltpu.roll(from_west, (-b) % LANES, 1) for b in range(OWN // STRIP)], axis=0
        )
        east_edge = jnp.concatenate(
            [pltpu.roll(from_east, (STRIP - 1 - b) % LANES, 1) for b in range(OWN // STRIP)], axis=0
        )
        west_side = jnp.where(wide_column == 0, west_edge, pltpu.roll(cell, 1, 1))
        east_side = jnp.where(wide_column == STRIP - 1, east_edge, pltpu.roll(cell, LANES - 1, 1))
        south_row = jnp.where(nest == 0, cell[0:1], rows_in[0, g, PR - 1 : PR])
        north_row = jnp.where(nest == NESTS - 1, cell[OWN - 1 : OWN], rows_in[1, g, 0:1])
        south_side = jnp.where(row == 0, south_row, pltpu.roll(cell, 1, 0))
        north_side = jnp.where(row == OWN - 1, north_row, pltpu.roll(cell, OWN - 1, 0))
        rate = jnp.full((1, LANES), rate_ref[g * GF], jnp.float32)
        for f in range(1, GF):
            rate = jnp.where(wide[0:1] // STRIP == f, rate_ref[g * GF + f], rate)
        new = cell + rate * (east_side + west_side + north_side + south_side - 4.0 * cell)
        out_ref[pl.ds(g * GF, GF)] = new.T.reshape(GF, STRIP, OWN)
        out_copy(g).start()

    for g in range(GROUPS):
        shift_rows(g)
        if g >= 1:
            merge(g - 1)
        if g >= 2:
            smooth(g - 2)
    smooth(GROUPS - 2)
    merge(GROUPS - 1)
    smooth(GROUPS - 1)

    for g in range(GROUPS):
        wait(slabs[g].at[pl.ds(0, NROWS - PR)], tile_send.at[g])
        for d in range(1, NESTS):
            nest_copy(g, d).wait_send()
        for copy in halo_copies(g):
            copy.wait_send()
        out_copy(g).wait()


def per_device(child_fields, row_weights, col_weights, nest_offsets, priority, parent_old, smooth_rate):
    hbm = pl.BlockSpec(memory_space=pl.ANY)
    f32, bf16 = jnp.float32, jnp.bfloat16
    dma = pltpu.SemaphoreType.DMA
    return pl.pallas_call(
        step_kernel,
        out_shape=jax.ShapeDtypeStruct(parent_old.shape, f32),
        in_specs=[hbm] * 7,
        out_specs=hbm,
        scratch_shapes=[
            pltpu.VMEM((32, 24, 3072), f32),
            pltpu.VMEM((3072, 1024), f32),
            pltpu.VMEM((256, 3072), bf16),
            pltpu.VMEM((128, 1024), f32),
            pltpu.VMEM((TILES, GROUPS, PR, LANES), f32),
            pltpu.VMEM((STRIP, OWN), jnp.int32),
            pltpu.VMEM((32, STRIP, OWN), f32),
            pltpu.VMEM((32, STRIP, OWN), f32),
            pltpu.SMEM((32,), f32),
            pltpu.SMEM((2, 4), jnp.int32),
            pltpu.VMEM((8, 24), f32),
            [pltpu.VMEM((NROWS + PR, LANES), f32)] * GROUPS,
            pltpu.VMEM((GROUPS, NROWS, LANES), f32),
            pltpu.VMEM((NESTS, GROUPS, OWN, LANES), f32),
            pltpu.VMEM((GROUPS, OWN, LANES), f32),
            pltpu.VMEM((OWN, LANES), f32),
            pltpu.VMEM((2, GROUPS, STRIP, LANES), f32),
            pltpu.VMEM((2, GROUPS, PR, LANES), f32),
            pltpu.VMEM((2, GROUPS, STRIP, LANES), f32),
            dma((GROUPS, 3)), dma((3072 // DEPTH,)), dma((5,)), dma((GROUPS,)),
            dma((GROUPS,)), dma((GROUPS,)), dma((GROUPS, NESTS)), dma((GROUPS, NESTS)),
            dma((GROUPS, 4)), dma((GROUPS, 4)),
        ],
        name="feedback",
        compiler_params=pltpu.CompilerParams(collective_id=0, has_side_effects=True),
    )(smooth_rate, nest_offsets.T, child_fields[0], row_weights, col_weights, priority, parent_old)


def solution(mesh):
    return jax.shard_map(
        per_device,
        mesh=mesh,
        in_specs=(
            P("nest", None, "tile", None), P(), P(), P(), P("tile", "nest"), P(None, "tile", "nest"), P(),
        ),
        out_specs=P(None, "tile", "nest"),
        check_vma=False,
    )
```
